16 devices in a mesh: dp: 1, tp: 16 (over x, y, z, core).
Axes of the slice: x: 2, y: 2, z: 2, core: 2. Of those that a mesh axis runs over, the one named last changes fastest.
Arguments:
- x: bfloat16 [2048, 7168], P('dp')
- w_gate: bfloat16 [7168, 20480], P(None, 'tp')
- w_up: bfloat16 [7168, 20480], P(None, 'tp')
- w_down: bfloat16 [20480, 7168], P('tp')
Outputs:
- output: bfloat16 [2048, 7168], P('dp')
All inputs are finite; a program needn't handle non-finite values.
Results may differ from the reference program's by a relative error of at most 0.016.
Values are sent between devices in bfloat16 or wider.
A program may use at most 2 GiB of HBM per device.

```python
import jax
import jax.numpy as jnp

ROWS = 2048
D = 7168
FF = 20480


def setup_inputs(seed: int = 0, part: int = 0) -> dict:
    kx, kg, ku, kd = jax.random.split(jax.random.key(seed), 4)
    drawn = {
        "x": jax.random.normal(jax.random.fold_in(kx, part), (ROWS, D), jnp.float32),
        "w_gate": jax.random.normal(kg, (D, FF), jnp.float32) * D**-0.5,
        "w_up": jax.random.normal(ku, (D, FF), jnp.float32) * D**-0.5,
        "w_down": jax.random.normal(kd, (FF, D), jnp.float32) * FF**-0.5,
    }
    return {k: v.astype(jnp.bfloat16) for k, v in drawn.items()}


def reference(x, w_gate, w_up, w_down):
    gate = jnp.dot(x, w_gate, preferred_element_type=jnp.float32)
    up = jnp.dot(x, w_up, preferred_element_type=jnp.float32)
    hidden = (jax.nn.silu(gate) * up).astype(jnp.bfloat16)
    return jnp.dot(hidden, w_down, preferred_element_type=jnp.float32).astype(jnp.bfloat16)
```

```python
import functools

import jax
import jax.numpy as jnp
from jax import lax
from jax.experimental import pallas as pl
from jax.experimental.pallas import tpu as pltpu
from jax.sharding import PartitionSpec as P

D = 7168
FF = 1280
M = 256
HALF = D // 2
OFF = (0, 1280, 2432)
WID = (1280, 1152, 1152)
GB = 256
NG = FF // GB
PC = M // 8
YS = 3
MESH = pl.DeviceIdType.MESH
F32 = jnp.float32
BF16 = jnp.bfloat16


def kernel(n, x_hbm, wg_hbm, wu_hbm, wd_hbm, y_hbm,
           xb, wgb, wub, wdb, hid, sb0, rb0, own, s1, r1, s2, r2, s3, r3, yo, yb,
           xsem, gsem, usem, dsem, osem,
           ss0, rs0, ss1, rs1, ss2, rs2, ss3, rs3, ssg, rsg, ssd, rsd):
    me = lax.axis_index("tp")
    core = me % 2
    sib = me + 1 - 2 * core
    bits = [(me // s) % 2 for s in (2, 4, 8)]
    prts = [me + s - 2 * s * ((me // s) % 2) for s in (2, 4, 8)]

    def pick(vals, axis):
        return (vals[0] * ((1 - axis) * (2 - axis) // 2) + vals[1] * (axis * (2 - axis))
                + vals[2] * (axis * (axis - 1) // 2))

    def geo(j, k):
        out = []
        for t in range(3):
            axis = (j + core + k + t) % 3
            out.append((pick(bits, axis), pick(prts, axis)))
        return out

    def rc(src, dst, ssem, rsem, dev):
        return pltpu.make_async_remote_copy(
            src_ref=src, dst_ref=dst, send_sem=ssem, recv_sem=rsem,
            device_id={"tp": dev}, device_id_type=MESH)

    def cols(k):
        return pl.ds(OFF[k], WID[k])

    def mo(v, m):
        return pl.multiple_of(v, m)

    def x_copy(i):
        return pltpu.make_async_copy(
            x_hbm.at[pl.ds(mo(i * M, M), M), :], xb.at[i % 2], xsem.at[i % 2])

    def g_copies(u):
        c = pl.ds(mo((u % NG) * GB, GB), GB)
        return (pltpu.make_async_copy(wg_hbm.at[:, c], wgb.at[u % 2], gsem.at[u % 2]),
                pltpu.make_async_copy(wu_hbm.at[:, c], wub.at[u % 2], usem.at[u % 2]))

    def d_copy(d):
        k = d % 3
        half = (1 - core) if d < 3 else core
        c = pl.ds(mo(half * HALF + OFF[k], 128), WID[k])
        return pltpu.make_async_copy(
            wd_hbm.at[:, c], wdb.at[d % 2, :, pl.ds(0, WID[k])], dsem.at[d % 2])

    def y_copy(j, buf, half, which):
        return pltpu.make_async_copy(
            buf.at[j % YS],
            y_hbm.at[pl.ds(mo(j * M, M), M), pl.ds(mo(half * HALF, 128), HALF)],
            osem.at[which, j % YS])

    def d2d0(j, k):
        return rc(sb0.at[:, cols(k)], rb0.at[j % 2, :, cols(k)], ss0.at[k], rs0.at[j % 2, k], sib)

    def off1(g, p):
        (_, _), (bb, _), (bc, _) = g
        if p == 0:
            return mo((1 - bb) * 2 * PC, PC), 2 * PC
        if p == 1:
            return mo(bb * 2 * PC + (1 - bc) * PC, PC), PC
        return mo(bb * 2 * PC + bc * PC, PC), PC

    def c1(j, k, g, p):
        o, r = off1(g, p)
        return rc(s1.at[pl.ds(o, r), cols(k)], r1.at[j % 2, pl.ds(o, r), cols(k)],
                  ss1.at[k, p], rs1.at[j % 2, k, p], g[0][1])

    def off2(g, p):
        bc = g[2][0]
        return mo((1 - bc) * PC if p == 0 else bc * PC, PC)

    def c2(j, k, g, p):
        o = off2(g, p)
        return rc(s2.at[pl.ds(o, PC), cols(k)], r2.at[j % 2, pl.ds(o, PC), cols(k)],
                  ss2.at[k, p], rs2.at[j % 2, k, p], g[1][1])

    def c3(j, k, g):
        return rc(s3.at[:, cols(k)], r3.at[j % 2, :, cols(k)], ss3.at[k], rs3.at[j % 2, k], g[2][1])

    AG = (((0, 0, 0), 2), ((0, 0, 0), 1), ((0, 0, 0), 0),
          ((0, 0, 1), 1), ((0, 0, 1), 0), ((0, 1, 0), 0), ((0, 1, 1), 0))

    def off_g(g, f):
        v = 0
        for t, wgt in enumerate((4, 2, 1)):
            b = g[t][0]
            v = v + (1 - b if f[t] else b) * (wgt * PC)
        return mo(v, PC)

    def cg(j, k, g, q):
        f, t = AG[q]
        o = off_g(g, f)
        ref = yo.at[j % YS, pl.ds(o, PC), cols(k)]
        return rc(ref, ref, ssg.at[j % YS, k, q], rsg.at[j % YS, k, q], g[t][1])

    def cg_in(j, k, g, q):
        f, t = AG[q]
        f = tuple(1 - v if u == t else v for u, v in enumerate(f))
        o = off_g(g, f)
        ref = yo.at[j % YS, pl.ds(o, PC), cols(k)]
        return rc(ref, ref, ssg.at[j % YS, k, q], rsg.at[j % YS, k, q], g[t][1])

    def cd(j, k, g, p, mine=True):
        ba = g[0][0]
        o = mo((ba if p == 0 else 1 - ba) * 4 * PC, 4 * PC)
        return rc(yo.at[j % YS, pl.ds(o, 4 * PC), cols(k)], yb.at[j % YS, pl.ds(o, 4 * PC), cols(k)],
                  ssd.at[j % YS, k, p], rsd.at[j % YS, k, p], sib)

    def cd_in(j, k, p):
        return rc(yo.at[j % YS, pl.ds(0, 4 * PC), cols(k)], yb.at[j % YS, pl.ds(0, 4 * PC), cols(k)],
                  ssd.at[j % YS, k, p], rsd.at[j % YS, k, p], sib)

    def stage1(i, k):
        g = geo(i, k)
        ba = g[0][0]
        o = mo((1 - ba) * 4 * PC, 4 * PC)
        s1[:, cols(k)] = own[pl.ds(o, 4 * PC), cols(k)].astype(BF16)
        for p in range(3):
            c1(i, k, g, p).start()

    def own_rows(g, o, r):
        return pl.ds(mo(g[0][0] * 4 * PC + o, PC), r)

    def stage2(j):
        for k in range(3):
            g = geo(j, k)
            o, r = off1(g, 0)
            c1(j, k, g, 0).wait_recv()
            s2[:, cols(k)] = (own[own_rows(g, o, r), cols(k)]
                              + r1[j % 2, pl.ds(o, r), cols(k)].astype(F32)).astype(BF16)
            for p in range(2):
                c2(j, k, g, p).start()
        for k in range(3):
            d2d0(j, k).wait_send()

    def stage3(j):
        for k in range(3):
            g = geo(j, k)
            o, r = off1(g, 1)
            c1(j, k, g, 1).wait_recv()
            c2(j, k, g, 0).wait_recv()
            s3[:, cols(k)] = (own[own_rows(g, o, r), cols(k)]
                              + r1[j % 2, pl.ds(o, r), cols(k)].astype(F32)
                              + r2[j % 2, pl.ds(off2(g, 0), PC), cols(k)].astype(F32)).astype(BF16)
            c3(j, k, g).start()

    def stage4(j):
        for k in range(3):
            g = geo(j, k)
            o, r = off1(g, 2)
            c1(j, k, g, 2).wait_recv()
            c2(j, k, g, 1).wait_recv()
            c3(j, k, g).wait_recv()
            yo[j % YS, pl.ds(off_g(g, (0, 0, 0)), PC), cols(k)] = (
                own[own_rows(g, o, r), cols(k)]
                + r1[j % 2, pl.ds(o, r), cols(k)].astype(F32)
                + r2[j % 2, pl.ds(off2(g, 1), PC), cols(k)].astype(F32)
                + r3[j % 2, :, cols(k)].astype(F32)).astype(BF16)
            for q in range(3):
                cg(j, k, g, q).start()
        for k in range(3):
            g = geo(j, k)
            for p in range(3):
                c1(j, k, g, p).wait_send()
            for p in range(2):
                c2(j, k, g, p).wait_send()
            c3(j, k, g).wait_send()

    def stage5(j):
        for k in range(3):
            g = geo(j, k)
            cg_in(j, k, g, 0).wait_recv()
            cg(j, k, g, 3).start()
            cg(j, k, g, 4).start()
            cg_in(j, k, g, 1).wait_recv()
            cg(j, k, g, 5).start()

    def stage6(j):
        for k in range(3):
            g = geo(j, k)
            cg_in(j, k, g, 3).wait_recv()
            cg(j, k, g, 6).start()
            cd(j, k, g, 0).start()

    def stage7(j):
        for k in range(3):
            g = geo(j, k)
            for q in (2, 4, 5, 6):
                cg_in(j, k, g, q).wait_recv()
            cd(j, k, g, 1).start()
        y_copy(j, yo, core, 0).start()

    def stage8(j):
        for k in range(3):
            for p in range(2):
                cd_in(j, k, p).wait_recv()
        y_copy(j, yb, 1 - core, 1).start()

    def stage9(j):
        for k in range(3):
            g = geo(j, k)
            for q in range(7):
                cg(j, k, g, q).wait_send()
            for p in range(2):
                cd(j, k, g, p).wait_send()
        y_copy(j, yo, core, 0).wait()
        y_copy(j, yb, 1 - core, 1).wait()

    def at(i, lag, stage):
        j = i - lag

        @pl.when((j >= 0) & (j < n))
        def _():
            stage(j)

    x_copy(0).start()
    for u in range(2):
        for c in g_copies(u):
            c.start()
    barrier = pltpu.get_barrier_semaphore()
    for dev in [sib] + prts:
        pl.semaphore_signal(barrier, inc=1, device_id={"tp": dev}, device_id_type=MESH)
    pl.semaphore_wait(barrier, 4)

    def slot(i, carry):
        at(i, 3, stage9)

        @pl.when(i < n)
        def _():
            x_copy(i).wait()

        def gate_up(b, carry):
            @pl.when(i < n)
            def _():
                u = NG * i + b
                for c in g_copies(u):
                    c.wait()
                gate = jnp.dot(xb[i % 2], wgb[u % 2], preferred_element_type=F32)
                up = jnp.dot(xb[i % 2], wub[u % 2], preferred_element_type=F32)
                hid[:, pl.ds(mo(b * GB, GB), GB)] = (jax.nn.silu(gate) * up).astype(BF16)

                @pl.when(u + 2 < NG * n)
                def _():
                    for c in g_copies(u + 2):
                        c.start()

                @pl.when((u == 1))
                def _():
                    d_copy(0).start()
                    d_copy(1).start()

                @pl.when((b == 3) & (i + 1 < n))
                def _():
                    x_copy(i + 1).start()

            for pos, lag, stage in ((0, 2, stage5), (1, 1, stage2), (2, 2, stage6),
                                    (3, 1, stage3), (4, 2, stage7)):
                @pl.when(b == pos)
                def _():
                    at(i, lag, stage)
            return carry

        lax.fori_loop(0, NG, gate_up, 0)

        def down(d):
            d_copy(d).wait()
            out = jnp.dot(hid[...], wdb[d % 2, :, :WID[d % 3]], preferred_element_type=F32)
            return out

        def next_down(d):
            if d + 2 < 6:
                d_copy(d + 2).start()
            else:
                @pl.when(i + 1 < n)
                def _():
                    d_copy(d - 4).start()

        for d in range(3):
            @pl.when(i < n)
            def _():
                sb0[:, cols(d)] = down(d).astype(BF16)
                d2d0(i, d).start()
                next_down(d)
        at(i, 1, stage4)
        at(i, 2, stage8)
        for d in range(3, 6):
            @pl.when(i < n)
            def _():
                k = d - 3
                d2d0(i, k).wait_recv()
                own[:, cols(k)] = down(d) + rb0[i % 2, :, cols(k)].astype(F32)
                stage1(i, k)
                next_down(d)
        return carry

    lax.fori_loop(0, n + 3, slot, 0)


def solution(mesh):
    def step(x, w_gate, w_up, w_down):
        n = x.shape[0] // M
        dma = pltpu.SemaphoreType.DMA
        return pl.pallas_call(
            functools.partial(kernel, n),
            out_shape=jax.ShapeDtypeStruct(x.shape, BF16),
            in_specs=[pl.BlockSpec(memory_space=pl.ANY)] * 4,
            out_specs=pl.BlockSpec(memory_space=pl.ANY),
            scratch_shapes=[
                pltpu.VMEM((2, M, D), BF16),
                pltpu.VMEM((2, D, GB), BF16),
                pltpu.VMEM((2, D, GB), BF16),
                pltpu.VMEM((2, FF, max(WID)), BF16),
                pltpu.VMEM((M, FF), BF16),
                pltpu.VMEM((M, HALF), BF16),
                pltpu.VMEM((2, M, HALF), BF16),
                pltpu.VMEM((M, HALF), F32),
                pltpu.VMEM((M // 2, HALF), BF16),
                pltpu.VMEM((2, M // 2, HALF), BF16),
                pltpu.VMEM((M // 4, HALF), BF16),
                pltpu.VMEM((2, M // 4, HALF), BF16),
                pltpu.VMEM((M // 8, HALF), BF16),
                pltpu.VMEM((2, M // 8, HALF), BF16),
                pltpu.VMEM((YS, M, HALF), BF16),
                pltpu.VMEM((YS, M, HALF), BF16),
                dma((2,)), dma((2,)), dma((2,)), dma((2,)), dma((2, YS)),
                dma((3,)), dma((2, 3)),
                dma((3, 3)), dma((2, 3, 3)),
                dma((3, 2)), dma((2, 3, 2)),
                dma((3,)), dma((2, 3)),
                dma((YS, 3, 7)), dma((YS, 3, 7)),
                dma((YS, 3, 2)), dma((YS, 3, 2)),
            ],
            compiler_params=pltpu.CompilerParams(
                collective_id=0, has_side_effects=True, vmem_limit_bytes=66_000_000),
            name="mlp_ring",
        )(x, w_gate, w_up, w_down)

    return jax.shard_map(
        step,
        mesh=mesh,
        in_specs=(P("dp", None), P(None, "tp"), P(None, "tp"), P("tp", None)),
        out_specs=P("dp", None),
        check_vma=False,
    )
```

```python
import functools

import jax
import jax.numpy as jnp
from jax import lax
from jax.experimental import pallas as pl
from jax.experimental.pallas import tpu as pltpu
from jax.sharding import PartitionSpec as P

D = 7168
FF = 1280
M = 256
HALF = D // 2
OFF = (0, 1280, 2432)
WID = (1280, 1152, 1152)
GB = 256
NG = FF // GB
PC = M // 8
YS = 3
MESH = pl.DeviceIdType.MESH
F32 = jnp.float32
BF16 = jnp.bfloat16


def kernel(n, x_hbm, wg_hbm, wu_hbm, wd_hbm, y_hbm,
           xb, wgb, wub, wdb, hid, sb0, rb0, own, s1, r1, s2, r2, s3, r3, yo, yb,
           xsem, gsem, usem, dsem, osem,
           ss0, rs0, ss1, rs1, ss2, rs2, ss3, rs3, ssg, rsg, ssd, rsd):
    me = lax.axis_index("tp")
    core = me % 2
    sib = me + 1 - 2 * core
    bits = [(me // s) % 2 for s in (2, 4, 8)]
    prts = [me + s - 2 * s * ((me // s) % 2) for s in (2, 4, 8)]

    def pick(vals, axis):
        return (vals[0] * ((1 - axis) * (2 - axis) // 2) + vals[1] * (axis * (2 - axis))
                + vals[2] * (axis * (axis - 1) // 2))

    def geo(j, k):
        out = []
        for t in range(3):
            axis = (j + core + k + t) % 3
            out.append((pick(bits, axis), pick(prts, axis)))
        return out

    def rc(src, dst, ssem, rsem, dev):
        return pltpu.make_async_remote_copy(
            src_ref=src, dst_ref=dst, send_sem=ssem, recv_sem=rsem,
            device_id={"tp": dev}, device_id_type=MESH)

    def cols(k):
        return pl.ds(OFF[k], WID[k])

    def mo(v, m):
        return pl.multiple_of(v, m)

    def x_copy(i):
        return pltpu.make_async_copy(
            x_hbm.at[pl.ds(mo(i * M, M), M), :], xb, xsem.at[0])

    def g_copies(u):
        c = pl.ds(mo((u % NG) * GB, GB), GB)
        return (pltpu.make_async_copy(wg_hbm.at[:, c], wgb.at[u % 2], gsem.at[u % 2]),
                pltpu.make_async_copy(wu_hbm.at[:, c], wub.at[u % 2], usem.at[u % 2]))

    def d_copy(d):
        k = d % 3
        half = (1 - core) if d < 3 else core
        c = pl.ds(mo(half * HALF + OFF[k], 128), WID[k])
        return pltpu.make_async_copy(wd_hbm.at[:, c], wdb.at[d // 3, :, cols(k)], dsem.at[d])

    def y_copy(j, buf, half, which):
        return pltpu.make_async_copy(
            buf.at[j % YS],
            y_hbm.at[pl.ds(mo(j * M, M), M), pl.ds(mo(half * HALF, 128), HALF)],
            osem.at[which, j % YS])

    def d2d0(j, k):
        return rc(sb0.at[:, cols(k)], rb0.at[j % 2, :, cols(k)], ss0.at[k], rs0.at[j % 2, k], sib)

    def off1(g, p):
        (_, _), (bb, _), (bc, _) = g
        if p == 0:
            return mo((1 - bb) * 2 * PC, PC), 2 * PC
        if p == 1:
            return mo(bb * 2 * PC + (1 - bc) * PC, PC), PC
        return mo(bb * 2 * PC + bc * PC, PC), PC

    def c1(j, k, g, p):
        o, r = off1(g, p)
        return rc(s1.at[pl.ds(o, r), cols(k)], r1.at[j % 2, pl.ds(o, r), cols(k)],
                  ss1.at[k, p], rs1.at[j % 2, k, p], g[0][1])

    def off2(g, p):
        bc = g[2][0]
        return mo((1 - bc) * PC if p == 0 else bc * PC, PC)

    def c2(j, k, g, p):
        o = off2(g, p)
        return rc(s2.at[pl.ds(o, PC), cols(k)], r2.at[j % 2, pl.ds(o, PC), cols(k)],
                  ss2.at[k, p], rs2.at[j % 2, k, p], g[1][1])

    def c3(j, k, g):
        return rc(s3.at[:, cols(k)], r3.at[j % 2, :, cols(k)], ss3.at[k], rs3.at[j % 2, k], g[2][1])

    AG = (((0, 0, 0), 2), ((0, 0, 0), 1), ((0, 0, 0), 0),
          ((0, 0, 1), 1), ((0, 0, 1), 0), ((0, 1, 0), 0), ((0, 1, 1), 0))

    def off_g(g, f):
        v = 0
        for t, wgt in enumerate((4, 2, 1)):
            b = g[t][0]
            v = v + (1 - b if f[t] else b) * (wgt * PC)
        return mo(v, PC)

    def cg(j, k, g, q):
        f, t = AG[q]
        o = off_g(g, f)
        ref = yo.at[j % YS, pl.ds(o, PC), cols(k)]
        return rc(ref, ref, ssg.at[j % YS, k, q], rsg.at[j % YS, k, q], g[t][1])

    def cg_in(j, k, g, q):
        f, t = AG[q]
        f = tuple(1 - v if u == t else v for u, v in enumerate(f))
        o = off_g(g, f)
        ref = yo.at[j % YS, pl.ds(o, PC), cols(k)]
        return rc(ref, ref, ssg.at[j % YS, k, q], rsg.at[j % YS, k, q], g[t][1])

    def cd(j, k, g, p, mine=True):
        ba = g[0][0]
        o = mo((ba if p == 0 else 1 - ba) * 4 * PC, 4 * PC)
        return rc(yo.at[j % YS, pl.ds(o, 4 * PC), cols(k)], yb.at[j % YS, pl.ds(o, 4 * PC), cols(k)],
                  ssd.at[j % YS, k, p], rsd.at[j % YS, k, p], sib)

    def cd_in(j, k, p):
        return rc(yo.at[j % YS, pl.ds(0, 4 * PC), cols(k)], yb.at[j % YS, pl.ds(0, 4 * PC), cols(k)],
                  ssd.at[j % YS, k, p], rsd.at[j % YS, k, p], sib)

    def stage1(i, k):
        g = geo(i, k)
        ba = g[0][0]
        o = mo((1 - ba) * 4 * PC, 4 * PC)
        s1[:, cols(k)] = own[pl.ds(o, 4 * PC), cols(k)].astype(BF16)
        for p in range(3):
            c1(i, k, g, p).start()

    def own_rows(g, o, r):
        return pl.ds(mo(g[0][0] * 4 * PC + o, PC), r)

    def stage2(j):
        for k in range(3):
            g = geo(j, k)
            o, r = off1(g, 0)
            c1(j, k, g, 0).wait_recv()
            s2[:, cols(k)] = (own[own_rows(g, o, r), cols(k)]
                              + r1[j % 2, pl.ds(o, r), cols(k)].astype(F32)).astype(BF16)
            for p in range(2):
                c2(j, k, g, p).start()
        for k in range(3):
            d2d0(j, k).wait_send()

    def stage3(j):
        for k in range(3):
            g = geo(j, k)
            o, r = off1(g, 1)
            c1(j, k, g, 1).wait_recv()
            c2(j, k, g, 0).wait_recv()
            s3[:, cols(k)] = (own[own_rows(g, o, r), cols(k)]
                              + r1[j % 2, pl.ds(o, r), cols(k)].astype(F32)
                              + r2[j % 2, pl.ds(off2(g, 0), PC), cols(k)].astype(F32)).astype(BF16)
            c3(j, k, g).start()

    def stage4(j):
        for k in range(3):
            g = geo(j, k)
            o, r = off1(g, 2)
            c1(j, k, g, 2).wait_recv()
            c2(j, k, g, 1).wait_recv()
            c3(j, k, g).wait_recv()
            yo[j % YS, pl.ds(off_g(g, (0, 0, 0)), PC), cols(k)] = (
                own[own_rows(g, o, r), cols(k)]
                + r1[j % 2, pl.ds(o, r), cols(k)].astype(F32)
                + r2[j % 2, pl.ds(off2(g, 1), PC), cols(k)].astype(F32)
                + r3[j % 2, :, cols(k)].astype(F32)).astype(BF16)
            for q in range(3):
                cg(j, k, g, q).start()
        for k in range(3):
            g = geo(j, k)
            for p in range(3):
                c1(j, k, g, p).wait_send()
            for p in range(2):
                c2(j, k, g, p).wait_send()
            c3(j, k, g).wait_send()

    def stage5(j):
        for k in range(3):
            g = geo(j, k)
            cg_in(j, k, g, 0).wait_recv()
            cg(j, k, g, 3).start()
            cg(j, k, g, 4).start()
            cg_in(j, k, g, 1).wait_recv()
            cg(j, k, g, 5).start()

    def stage6(j):
        for k in range(3):
            g = geo(j, k)
            cg_in(j, k, g, 3).wait_recv()
            cg(j, k, g, 6).start()
            cd(j, k, g, 0).start()

    def stage7(j):
        for k in range(3):
            g = geo(j, k)
            for q in (2, 4, 5, 6):
                cg_in(j, k, g, q).wait_recv()
            cd(j, k, g, 1).start()
        y_copy(j, yo, core, 0).start()

    def stage8(j):
        for k in range(3):
            for p in range(2):
                cd_in(j, k, p).wait_recv()
        y_copy(j, yb, 1 - core, 1).start()

    def stage9(j):
        for k in range(3):
            g = geo(j, k)
            for q in range(7):
                cg(j, k, g, q).wait_send()
            for p in range(2):
                cd(j, k, g, p).wait_send()
        y_copy(j, yo, core, 0).wait()
        y_copy(j, yb, 1 - core, 1).wait()

    def at(i, lag, stage):
        j = i - lag

        @pl.when((j >= 0) & (j < n))
        def _():
            stage(j)

    x_copy(0).start()
    for u in range(2):
        for c in g_copies(u):
            c.start()
    barrier = pltpu.get_barrier_semaphore()
    for dev in [sib] + prts:
        pl.semaphore_signal(barrier, inc=1, device_id={"tp": dev}, device_id_type=MESH)
    pl.semaphore_wait(barrier, 4)

    def slot(i, carry):
        @pl.when(i < n)
        def _():
            x_copy(i).wait()

        def gate_up(b, carry):
            @pl.when(i < n)
            def _():
                u = NG * i + b
                for c in g_copies(u):
                    c.wait()
                gate = jnp.dot(xb[...], wgb[u % 2], preferred_element_type=F32)
                up = jnp.dot(xb[...], wub[u % 2], preferred_element_type=F32)
                hid[:, pl.ds(mo(b * GB, GB), GB)] = (jax.nn.silu(gate) * up).astype(BF16)

                @pl.when(u + 2 < NG * n)
                def _():
                    for c in g_copies(u + 2):
                        c.start()

                for p, ds in ((1, (0,)), (2, (1,)), (3, (2,)), (4, (3, 4, 5))):
                    @pl.when(u == p)
                    def _():
                        for d in ds:
                            d_copy(d).start()

                @pl.when((b == NG - 1) & (i + 1 < n))
                def _():
                    x_copy(i + 1).start()

            for pos, lag, stage in ((1, 1, stage2), (2, 2, stage5), (2, 3, stage8),
                                    (3, 1, stage3), (4, 2, stage6), (4, 3, stage9)):
                @pl.when(b == pos)
                def _():
                    at(i, lag, stage)
            return carry

        lax.fori_loop(0, NG, gate_up, 0)

        def down(d):
            @pl.when(i == 0)
            def _():
                d_copy(d).wait()
            return jnp.dot(hid[...], wdb[d // 3, :, cols(d % 3)], preferred_element_type=F32)

        for d in range(3):
            @pl.when(i < n)
            def _():
                sb0[:, cols(d)] = down(d).astype(BF16)
                d2d0(i, d).start()
            if d == 0:
                at(i, 1, stage4)
        for k in range(3):
            @pl.when(i < n)
            def _():
                d2d0(i, k).wait_recv()
                own[:, cols(k)] = down(3 + k) + rb0[i % 2, :, cols(k)].astype(F32)
                stage1(i, k)
        at(i, 2, stage7)
        return carry

    lax.fori_loop(0, n + 3, slot, 0)


def solution(mesh):
    def step(x, w_gate, w_up, w_down):
        n = x.shape[0] // M
        dma = pltpu.SemaphoreType.DMA
        return pl.pallas_call(
            functools.partial(kernel, n),
            out_shape=jax.ShapeDtypeStruct(x.shape, BF16),
            in_specs=[pl.BlockSpec(memory_space=pl.ANY)] * 4,
            out_specs=pl.BlockSpec(memory_space=pl.ANY),
            scratch_shapes=[
                pltpu.VMEM((M, D), BF16),
                pltpu.VMEM((2, D, GB), BF16),
                pltpu.VMEM((2, D, GB), BF16),
                pltpu.VMEM((2, FF, HALF), BF16),
                pltpu.VMEM((M, FF), BF16),
                pltpu.VMEM((M, HALF), BF16),
                pltpu.VMEM((2, M, HALF), BF16),
                pltpu.VMEM((M, HALF), F32),
                pltpu.VMEM((M // 2, HALF), BF16),
                pltpu.VMEM((2, M // 2, HALF), BF16),
                pltpu.VMEM((M // 4, HALF), BF16),
                pltpu.VMEM((2, M // 4, HALF), BF16),
                pltpu.VMEM((M // 8, HALF), BF16),
                pltpu.VMEM((2, M // 8, HALF), BF16),
                pltpu.VMEM((YS, M, HALF), BF16),
                pltpu.VMEM((YS, M, HALF), BF16),
                dma((1,)), dma((2,)), dma((2,)), dma((6,)), dma((2, YS)),
                dma((3,)), dma((2, 3)),
                dma((3, 3)), dma((2, 3, 3)),
                dma((3, 2)), dma((2, 3, 2)),
                dma((3,)), dma((2, 3)),
                dma((YS, 3, 7)), dma((YS, 3, 7)),
                dma((YS, 3, 2)), dma((YS, 3, 2)),
            ],
            compiler_params=pltpu.CompilerParams(
                collective_id=0, has_side_effects=True, vmem_limit_bytes=67_043_328),
            name="mlp_ring",
        )(x, w_gate, w_up, w_down)

    return jax.shard_map(
        step,
        mesh=mesh,
        in_specs=(P("dp", None), P(None, "tp"), P(None, "tp"), P("tp", None)),
        out_specs=P("dp", None),
        check_vma=False,
    )
```

```python
import functools

import jax
import jax.numpy as jnp
from jax import lax
from jax.experimental import pallas as pl
from jax.experimental.pallas import tpu as pltpu
from jax.sharding import PartitionSpec as P

D = 7168
FF = 1280
M = 256
HALF = D // 2
OFF = (0, 1280, 2432)
WID = (1280, 1152, 1152)
GB = 256
NG = FF // GB
DH = D // 2
GS = 3
PC = M // 8
YS = 3
MESH = pl.DeviceIdType.MESH
F32 = jnp.float32
BF16 = jnp.bfloat16


def kernel(n, x_hbm, wg_hbm, wu_hbm, wd_hbm, t_hbm, wdb, yo, yb,
           xb, wgb, wub, hid, sb0, rb0, own, s1, r1, s2, r2, s3, r3,
           xsem, gsem, usem, dsem, osem,
           ss0, rs0, ss1, rs1, ss2, rs2, ss3, rs3, ssg, rsg, ssd, rsd):
    me = lax.axis_index("tp")
    core = me % 2
    sib = me + 1 - 2 * core
    bits = [(me // s) % 2 for s in (2, 4, 8)]
    prts = [me + s - 2 * s * ((me // s) % 2) for s in (2, 4, 8)]

    def pick(vals, axis):
        return (vals[0] * ((1 - axis) * (2 - axis) // 2) + vals[1] * (axis * (2 - axis))
                + vals[2] * (axis * (axis - 1) // 2))

    def geo(j, k):
        out = []
        for t in range(3):
            axis = (j + core + k + t) % 3
            out.append((pick(bits, axis), pick(prts, axis)))
        return out

    def rc(src, dst, ssem, rsem, dev):
        return pltpu.make_async_remote_copy(
            src_ref=src, dst_ref=dst, send_sem=ssem, recv_sem=rsem,
            device_id={"tp": dev}, device_id_type=MESH)

    def cols(k):
        return pl.ds(OFF[k], WID[k])

    def mo(v, m):
        return pl.multiple_of(v, m)

    def x_copy(i):
        return pltpu.make_async_copy(
            x_hbm.at[pl.ds(mo(i * M, M), M), :], xb, xsem.at[0])

    def g_copies(v):
        c = pl.ds(mo((v // 2) % NG * GB, GB), GB)
        r = pl.ds(mo(v % 2 * DH, DH), DH)
        return (pltpu.make_async_copy(wg_hbm.at[r, c], wgb.at[v % GS], gsem.at[v % GS]),
                pltpu.make_async_copy(wu_hbm.at[r, c], wub.at[v % GS], usem.at[v % GS]))

    def d_copy(d):
        k = d % 3
        half = (1 - core) if d < 3 else core
        c = pl.ds(mo(half * HALF + OFF[k], 128), WID[k])
        return pltpu.make_async_copy(wd_hbm.at[:, c], wdb.at[d // 3, :, cols(k)], dsem.at[d])

    def y_copy(j, buf, half, which):
        return pltpu.make_async_copy(
            buf.at[j % YS], t_hbm.at[half, pl.ds(mo(j * M, M), M), :], osem.at[which, j % YS])

    def t_copy(h):
        r = (n - YS) * M
        return pltpu.make_async_copy(t_hbm.at[h], wdb.at[h, pl.ds(0, r), :], dsem.at[h])

    def d2d0(j, k):
        return rc(sb0.at[:, cols(k)], rb0.at[j % 2, :, cols(k)], ss0.at[k], rs0.at[j % 2, k], sib)

    def off1(g, p):
        (_, _), (bb, _), (bc, _) = g
        if p == 0:
            return mo((1 - bb) * 2 * PC, PC), 2 * PC
        if p == 1:
            return mo(bb * 2 * PC + (1 - bc) * PC, PC), PC
        return mo(bb * 2 * PC + bc * PC, PC), PC

    def c1(j, k, g, p):
        o, r = off1(g, p)
        return rc(s1.at[pl.ds(o, r), cols(k)], r1.at[j % 2, pl.ds(o, r), cols(k)],
                  ss1.at[k, p], rs1.at[j % 2, k, p], g[0][1])

    def off2(g, p):
        bc = g[2][0]
        return mo((1 - bc) * PC if p == 0 else bc * PC, PC)

    def c2(j, k, g, p):
        o = off2(g, p)
        return rc(s2.at[pl.ds(o, PC), cols(k)], r2.at[j % 2, pl.ds(o, PC), cols(k)],
                  ss2.at[k, p], rs2.at[j % 2, k, p], g[1][1])

    def c3(j, k, g):
        return rc(s3.at[:, cols(k)], r3.at[j % 2, :, cols(k)], ss3.at[k], rs3.at[j % 2, k], g[2][1])

    AG = (((0, 0, 0), 2), ((0, 0, 0), 1), ((0, 0, 0), 0),
          ((0, 0, 1), 1), ((0, 0, 1), 0), ((0, 1, 0), 0), ((0, 1, 1), 0))

    def off_g(g, f):
        v = 0
        for t, wgt in enumerate((4, 2, 1)):
            b = g[t][0]
            v = v + (1 - b if f[t] else b) * (wgt * PC)
        return mo(v, PC)

    def cg(j, k, g, q):
        f, t = AG[q]
        o = off_g(g, f)
        ref = yo.at[j % YS, pl.ds(o, PC), cols(k)]
        return rc(ref, ref, ssg.at[j % YS, k, q], rsg.at[j % YS, k, q], g[t][1])

    def cg_in(j, k, g, q):
        f, t = AG[q]
        f = tuple(1 - v if u == t else v for u, v in enumerate(f))
        o = off_g(g, f)
        ref = yo.at[j % YS, pl.ds(o, PC), cols(k)]
        return rc(ref, ref, ssg.at[j % YS, k, q], rsg.at[j % YS, k, q], g[t][1])

    def cd(j, k, g, p, mine=True):
        ba = g[0][0]
        o = mo((ba if p == 0 else 1 - ba) * 4 * PC, 4 * PC)
        return rc(yo.at[j % YS, pl.ds(o, 4 * PC), cols(k)], yb.at[j % YS, pl.ds(o, 4 * PC), cols(k)],
                  ssd.at[j % YS, k, p], rsd.at[j % YS, k, p], sib)

    def cd_in(j, k, p):
        return rc(yo.at[j % YS, pl.ds(0, 4 * PC), cols(k)], yb.at[j % YS, pl.ds(0, 4 * PC), cols(k)],
                  ssd.at[j % YS, k, p], rsd.at[j % YS, k, p], sib)

    def stage1(i, k):
        g = geo(i, k)
        ba = g[0][0]
        o = mo((1 - ba) * 4 * PC, 4 * PC)
        s1[:, cols(k)] = own[pl.ds(o, 4 * PC), cols(k)].astype(BF16)
        for p in range(3):
            c1(i, k, g, p).start()

    def own_rows(g, o, r):
        return pl.ds(mo(g[0][0] * 4 * PC + o, PC), r)

    def stage2(j):
        for k in range(3):
            g = geo(j, k)
            o, r = off1(g, 0)
            c1(j, k, g, 0).wait_recv()
            s2[:, cols(k)] = (own[own_rows(g, o, r), cols(k)]
                              + r1[j % 2, pl.ds(o, r), cols(k)].astype(F32)).astype(BF16)
            for p in range(2):
                c2(j, k, g, p).start()
        for k in range(3):
            d2d0(j, k).wait_send()

    def stage3(j):
        for k in range(3):
            g = geo(j, k)
            o, r = off1(g, 1)
            c1(j, k, g, 1).wait_recv()
            c2(j, k, g, 0).wait_recv()
            s3[:, cols(k)] = (own[own_rows(g, o, r), cols(k)]
                              + r1[j % 2, pl.ds(o, r), cols(k)].astype(F32)
                              + r2[j % 2, pl.ds(off2(g, 0), PC), cols(k)].astype(F32)).astype(BF16)
            c3(j, k, g).start()

    def stage4(j):
        for k in range(3):
            g = geo(j, k)
            o, r = off1(g, 2)
            c1(j, k, g, 2).wait_recv()
            c2(j, k, g, 1).wait_recv()
            c3(j, k, g).wait_recv()
            yo[j % YS, pl.ds(off_g(g, (0, 0, 0)), PC), cols(k)] = (
                own[own_rows(g, o, r), cols(k)]
                + r1[j % 2, pl.ds(o, r), cols(k)].astype(F32)
                + r2[j % 2, pl.ds(off2(g, 1), PC), cols(k)].astype(F32)
                + r3[j % 2, :, cols(k)].astype(F32)).astype(BF16)
            for q in range(3):
                cg(j, k, g, q).start()
        for k in range(3):
            g = geo(j, k)
            for p in range(3):
                c1(j, k, g, p).wait_send()
            for p in range(2):
                c2(j, k, g, p).wait_send()
            c3(j, k, g).wait_send()

    def stage5(j):
        for k in range(3):
            g = geo(j, k)
            cg_in(j, k, g, 0).wait_recv()
            cg(j, k, g, 3).start()
            cg(j, k, g, 4).start()
            cg_in(j, k, g, 1).wait_recv()
            cg(j, k, g, 5).start()

    def stage6(j):
        for k in range(3):
            g = geo(j, k)
            cg_in(j, k, g, 3).wait_recv()
            cg(j, k, g, 6).start()
            cd(j, k, g, 0).start()

    def stage7(j):
        for k in range(3):
            g = geo(j, k)
            for q in (2, 4, 5, 6):
                cg_in(j, k, g, q).wait_recv()
            cd(j, k, g, 1).start()

        @pl.when(j < n - YS)
        def _():
            y_copy(j, yo, core, 0).start()

    def stage8(j):
        for k in range(3):
            for p in range(2):
                cd_in(j, k, p).wait_recv()

        @pl.when(j < n - YS)
        def _():
            y_copy(j, yb, 1 - core, 1).start()

    def stage9(j):
        for k in range(3):
            g = geo(j, k)
            for q in range(7):
                cg(j, k, g, q).wait_send()
            for p in range(2):
                cd(j, k, g, p).wait_send()

        @pl.when(j < n - YS)
        def _():
            y_copy(j, yo, core, 0).wait()
            y_copy(j, yb, 1 - core, 1).wait()

    def at(i, lag, stage):
        j = i - lag

        @pl.when((j >= 0) & (j < n))
        def _():
            stage(j)

    x_copy(0).start()
    for v in range(GS):
        for c in g_copies(v):
            c.start()
    barrier = pltpu.get_barrier_semaphore()
    for dev in [sib] + prts:
        pl.semaphore_signal(barrier, inc=1, device_id={"tp": dev}, device_id_type=MESH)
    pl.semaphore_wait(barrier, 4)

    def slot(i, carry):
        @pl.when(i < n)
        def _():
            x_copy(i).wait()

        @pl.when(i == n)
        def _():
            for h in range(2):
                t_copy(h).start()

        def gate_up(b, carry):
            @pl.when(i < n)
            def _():
                u = NG * i + b
                gate = up = 0.0
                for h in range(2):
                    v = 2 * u + h
                    for c in g_copies(v):
                        c.wait()
                    xh = xb[:, h * DH:(h + 1) * DH]
                    gate += jnp.dot(xh, wgb[v % GS], preferred_element_type=F32)
                    up += jnp.dot(xh, wub[v % GS], preferred_element_type=F32)

                    @pl.when((v + GS < 2 * NG * n) & ((i > 0) | (v + GS < 2 * NG)))
                    def _():
                        for c in g_copies(v + GS):
                            c.start()
                hid[:, pl.ds(mo(b * GB, GB), GB)] = (jax.nn.silu(gate) * up).astype(BF16)

                for p, ds in ((2, (0, 1)), (3, (2, 3)), (4, (4, 5))):
                    @pl.when(u == p)
                    def _():
                        for d in ds:
                            d_copy(d).start()

                @pl.when((b == NG - 1) & (i > 0) & (i + 1 < n))
                def _():
                    x_copy(i + 1).start()

            for pos, lag, stage in ((1, 1, stage2), (1, 3, stage6), (3, 1, stage3),
                                    (3, 2, stage5), (3, 3, stage7), (4, 3, stage8)):
                @pl.when(b == pos)
                def _():
                    at(i, lag, stage)
            return carry

        lax.fori_loop(0, NG, gate_up, 0)

        def down(d):
            @pl.when(i == 0)
            def _():
                d_copy(d).wait()
            return jnp.dot(hid[...], wdb[d // 3, :, cols(d % 3)], preferred_element_type=F32)

        for d in range(3):
            @pl.when(i < n)
            def _():
                sb0[:, cols(d)] = down(d).astype(BF16)
                d2d0(i, d).start()
            if d == 0:
                at(i, 3, stage9)
                at(i, 1, stage4)

        @pl.when(i == 0)
        def _():
            x_copy(1).start()
            for v in range(2 * NG, 2 * NG + GS):
                for c in g_copies(v):
                    c.start()

        for k in range(3):
            @pl.when(i < n)
            def _():
                d2d0(i, k).wait_recv()
                own[:, cols(k)] = down(3 + k) + rb0[i % 2, :, cols(k)].astype(F32)
                stage1(i, k)
        return carry

    lax.fori_loop(0, n + 3, slot, 0)
    for h in range(2):
        t_copy(h).wait()


def finish(n, wdb, yo, yb, y_hbm, sem):
    core = lax.axis_index("tp") % 2
    outs = []
    for j in range(n):
        for h in range(2):
            rows = pl.ds(j * M, M)
            if j < n - YS:
                src, half = wdb.at[h, rows, :], h
            else:
                src, half = (yo, yb)[h].at[j % YS], (core, 1 - core)[h]
            dst = y_hbm.at[rows, pl.ds(pl.multiple_of(half * HALF, 128), HALF)]
            outs.append(pltpu.make_async_copy(src, dst, sem.at[j, h]))
            outs[-1].start()
    for c in outs:
        c.wait()


def solution(mesh):
    def step(x, w_gate, w_up, w_down):
        n = x.shape[0] // M
        assert n > YS and (n - YS) * M <= FF
        dma = pltpu.SemaphoreType.DMA
        vmem = pl.BlockSpec(memory_space=pltpu.VMEM)
        part = pltpu.VMEM((YS, M, HALF), BF16)
        outs = pl.pallas_call(
            functools.partial(kernel, n),
            out_shape=(jax.ShapeDtypeStruct((2, (n - YS) * M, HALF), BF16),
                       pltpu.VMEM((2, FF, HALF), BF16), part, part),
            in_specs=[pl.BlockSpec(memory_space=pl.ANY)] * 4,
            out_specs=(pl.BlockSpec(memory_space=pl.ANY), vmem, vmem, vmem),
            scratch_shapes=[
                pltpu.VMEM((M, D), BF16),
                pltpu.VMEM((GS, DH, GB), BF16),
                pltpu.VMEM((GS, DH, GB), BF16),
                pltpu.VMEM((M, FF), BF16),
                pltpu.VMEM((M, HALF), BF16),
                pltpu.VMEM((2, M, HALF), BF16),
                pltpu.VMEM((M, HALF), F32),
                pltpu.VMEM((M // 2, HALF), BF16),
                pltpu.VMEM((2, M // 2, HALF), BF16),
                pltpu.VMEM((M // 4, HALF), BF16),
                pltpu.VMEM((2, M // 4, HALF), BF16),
                pltpu.VMEM((M // 8, HALF), BF16),
                pltpu.VMEM((2, M // 8, HALF), BF16),
                dma((1,)), dma((GS,)), dma((GS,)), dma((6,)), dma((2, YS)),
                dma((3,)), dma((2, 3)),
                dma((3, 3)), dma((2, 3, 3)),
                dma((3, 2)), dma((2, 3, 2)),
                dma((3,)), dma((2, 3)),
                dma((YS, 3, 7)), dma((YS, 3, 7)),
                dma((YS, 3, 2)), dma((YS, 3, 2)),
            ],
            compiler_params=pltpu.CompilerParams(
                collective_id=0, has_side_effects=True, vmem_limit_bytes=37_500_000),
            name="mlp_ring",
        )(x, w_gate, w_up, w_down)
        return pl.pallas_call(
            functools.partial(finish, n),
            out_shape=jax.ShapeDtypeStruct(x.shape, BF16),
            in_specs=[vmem] * 3,
            out_specs=pl.BlockSpec(memory_space=pl.ANY),
            scratch_shapes=[dma((n, 2))],
            compiler_params=pltpu.CompilerParams(vmem_limit_bytes=1_000_000),
            name="finish",
        )(*outs[1:])

    return jax.shard_map(
        step,
        mesh=mesh,
        in_specs=(P("dp", None), P(None, "tp"), P(None, "tp"), P("tp", None)),
        out_specs=P("dp", None),
        check_vma=False,
    )
```

```python
import functools

import jax
import jax.numpy as jnp
from jax import lax
from jax.experimental import pallas as pl
from jax.experimental.pallas import tpu as pltpu
from jax.sharding import PartitionSpec as P

D = 7168
FF = 1280
M = 256
HALF = D // 2
OFF = (0, 1280, 2432)
WID = (1280, 1152, 1152)
GB = 256
NG = FF // GB
DH = D // 2
GS = 3
PC = M // 8
YS = 3
MESH = pl.DeviceIdType.MESH
F32 = jnp.float32
BF16 = jnp.bfloat16


def kernel(n, x_hbm, wg_hbm, wu_hbm, wd_hbm, t_hbm, wdb, yo, yb,
           xb, wgb, wub, hid, sb0, rb0, own, s1, r1, s2, r2, s3, r3,
           xsem, gsem, usem, dsem, osem,
           ss0, rs0, ss1, rs1, ss2, rs2, ss3, rs3, ssg, rsg, ssd, rsd):
    me = lax.axis_index("tp")
    core = me % 2
    sib = me + 1 - 2 * core
    bits = [(me // s) % 2 for s in (2, 4, 8)]
    prts = [me + s - 2 * s * ((me // s) % 2) for s in (2, 4, 8)]

    def pick(vals, axis):
        return (vals[0] * ((1 - axis) * (2 - axis) // 2) + vals[1] * (axis * (2 - axis))
                + vals[2] * (axis * (axis - 1) // 2))

    def geo(j, k):
        out = []
        for t in range(3):
            axis = (j + core + k + t) % 3
            out.append((pick(bits, axis), pick(prts, axis)))
        return out

    def rc(src, dst, ssem, rsem, dev):
        return pltpu.make_async_remote_copy(
            src_ref=src, dst_ref=dst, send_sem=ssem, recv_sem=rsem,
            device_id={"tp": dev}, device_id_type=MESH)

    def cols(k):
        return pl.ds(OFF[k], WID[k])

    def mo(v, m):
        return pl.multiple_of(v, m)

    def x_copy(i):
        return pltpu.make_async_copy(
            x_hbm.at[pl.ds(mo(i * M, M), M), :], xb, xsem.at[0])

    def g_copies(v):
        c = pl.ds(mo((v // 2) % NG * GB, GB), GB)
        r = pl.ds(mo(v % 2 * DH, DH), DH)
        return (pltpu.make_async_copy(wg_hbm.at[r, c], wgb.at[v % GS], gsem.at[v % GS]),
                pltpu.make_async_copy(wu_hbm.at[r, c], wub.at[v % GS], usem.at[v % GS]))

    def d_copy(d):
        k = d % 3
        half = (1 - core) if d < 3 else core
        c = pl.ds(mo(half * HALF + OFF[k], 128), WID[k])
        return pltpu.make_async_copy(wd_hbm.at[:, c], wdb.at[d // 3, :, cols(k)], dsem.at[d])

    def y_copy(j, buf, half, which):
        return pltpu.make_async_copy(
            buf.at[j % YS], t_hbm.at[half, pl.ds(mo(j * M, M), M), :], osem.at[which, j % YS])

    def t_copy(h):
        r = (n - YS) * M
        return pltpu.make_async_copy(t_hbm.at[h], wdb.at[h, pl.ds(0, r), :], dsem.at[h])

    def d2d0(j, k):
        return rc(sb0.at[:, cols(k)], rb0.at[j % 2, :, cols(k)], ss0.at[k], rs0.at[j % 2, k], sib)

    def off1(g, p):
        (_, _), (bb, _), (bc, _) = g
        if p == 0:
            return mo((1 - bb) * 2 * PC, PC), 2 * PC
        if p == 1:
            return mo(bb * 2 * PC + (1 - bc) * PC, PC), PC
        return mo(bb * 2 * PC + bc * PC, PC), PC

    def c1(j, k, g, p):
        o, r = off1(g, p)
        return rc(s1.at[pl.ds(o, r), cols(k)], r1.at[j % 2, pl.ds(o, r), cols(k)],
                  ss1.at[k, p], rs1.at[j % 2, k, p], g[0][1])

    def off2(g, p):
        bc = g[2][0]
        return mo((1 - bc) * PC if p == 0 else bc * PC, PC)

    def c2(j, k, g, p):
        o = off2(g, p)
        return rc(s2.at[pl.ds(o, PC), cols(k)], r2.at[j % 2, pl.ds(o, PC), cols(k)],
                  ss2.at[k, p], rs2.at[j % 2, k, p], g[1][1])

    def c3(j, k, g):
        return rc(s3.at[:, cols(k)], r3.at[j % 2, :, cols(k)], ss3.at[k], rs3.at[j % 2, k], g[2][1])

    AG = (((0, 0, 0), 2), ((0, 0, 0), 1), ((0, 0, 0), 0),
          ((0, 0, 1), 1), ((0, 0, 1), 0), ((0, 1, 0), 0), ((0, 1, 1), 0))

    def off_g(g, f):
        v = 0
        for t, wgt in enumerate((4, 2, 1)):
            b = g[t][0]
            v = v + (1 - b if f[t] else b) * (wgt * PC)
        return mo(v, PC)

    def cg(j, k, g, q):
        f, t = AG[q]
        o = off_g(g, f)
        ref = yo.at[j % YS, pl.ds(o, PC), cols(k)]
        return rc(ref, ref, ssg.at[j % YS, k, q], rsg.at[j % YS, k, q], g[t][1])

    def cg_in(j, k, g, q):
        f, t = AG[q]
        f = tuple(1 - v if u == t else v for u, v in enumerate(f))
        o = off_g(g, f)
        ref = yo.at[j % YS, pl.ds(o, PC), cols(k)]
        return rc(ref, ref, ssg.at[j % YS, k, q], rsg.at[j % YS, k, q], g[t][1])

    def cd(j, k, g, p, mine=True):
        ba = g[0][0]
        o = mo((ba if p == 0 else 1 - ba) * 4 * PC, 4 * PC)
        return rc(yo.at[j % YS, pl.ds(o, 4 * PC), cols(k)], yb.at[j % YS, pl.ds(o, 4 * PC), cols(k)],
                  ssd.at[j % YS, k, p], rsd.at[j % YS, k, p], sib)

    def cd_in(j, k, p):
        return rc(yo.at[j % YS, pl.ds(0, 4 * PC), cols(k)], yb.at[j % YS, pl.ds(0, 4 * PC), cols(k)],
                  ssd.at[j % YS, k, p], rsd.at[j % YS, k, p], sib)

    def stage1(i, k):
        g = geo(i, k)
        ba = g[0][0]
        o = mo((1 - ba) * 4 * PC, 4 * PC)
        s1[:, cols(k)] = own[pl.ds(o, 4 * PC), cols(k)].astype(BF16)
        for p in range(3):
            c1(i, k, g, p).start()

    def own_rows(g, o, r):
        return pl.ds(mo(g[0][0] * 4 * PC + o, PC), r)

    def stage2(j, k):
        g = geo(j, k)
        o, r = off1(g, 0)
        c1(j, k, g, 0).wait_recv()
        s2[:, cols(k)] = (own[own_rows(g, o, r), cols(k)]
                          + r1[j % 2, pl.ds(o, r), cols(k)].astype(F32)).astype(BF16)
        for p in range(2):
            c2(j, k, g, p).start()
        d2d0(j, k).wait_send()

    def stage3(j, k):
        g = geo(j, k)
        o, r = off1(g, 1)
        c1(j, k, g, 1).wait_recv()
        c2(j, k, g, 0).wait_recv()
        s3[:, cols(k)] = (own[own_rows(g, o, r), cols(k)]
                          + r1[j % 2, pl.ds(o, r), cols(k)].astype(F32)
                          + r2[j % 2, pl.ds(off2(g, 0), PC), cols(k)].astype(F32)).astype(BF16)
        c3(j, k, g).start()

    def stage4(j, k):
        g = geo(j, k)
        o, r = off1(g, 2)
        c1(j, k, g, 2).wait_recv()
        c2(j, k, g, 1).wait_recv()
        c3(j, k, g).wait_recv()
        yo[j % YS, pl.ds(off_g(g, (0, 0, 0)), PC), cols(k)] = (
            own[own_rows(g, o, r), cols(k)]
            + r1[j % 2, pl.ds(o, r), cols(k)].astype(F32)
            + r2[j % 2, pl.ds(off2(g, 1), PC), cols(k)].astype(F32)
            + r3[j % 2, :, cols(k)].astype(F32)).astype(BF16)
        for q in range(3):
            cg(j, k, g, q).start()
        for p in range(3):
            c1(j, k, g, p).wait_send()
        for p in range(2):
            c2(j, k, g, p).wait_send()
        c3(j, k, g).wait_send()

    def stage5(j, k):
        g = geo(j, k)
        cg_in(j, k, g, 0).wait_recv()
        cg(j, k, g, 3).start()
        cg(j, k, g, 4).start()
        cg_in(j, k, g, 1).wait_recv()
        cg(j, k, g, 5).start()

    def stage6(j, k):
        g = geo(j, k)
        cg_in(j, k, g, 3).wait_recv()
        cg(j, k, g, 6).start()
        cd(j, k, g, 0).start()

    def stage7(j, k):
        g = geo(j, k)
        for q in (2, 4, 5, 6):
            cg_in(j, k, g, q).wait_recv()
        cd(j, k, g, 1).start()

    def stage8(j, k):
        for p in range(2):
            cd_in(j, k, p).wait_recv()

    def store(j, which):
        @pl.when(j < n - YS)
        def _():
            y_copy(j, (yo, yb)[which], (core, 1 - core)[which], which).start()

    def stage9(j, _):
        for k in range(3):
            g = geo(j, k)
            for q in range(7):
                cg(j, k, g, q).wait_send()
            for p in range(2):
                cd(j, k, g, p).wait_send()

        @pl.when(j < n - YS)
        def _():
            y_copy(j, yo, core, 0).wait()
            y_copy(j, yb, 1 - core, 1).wait()

    plan = {
        1: ((1, stage2, 1), (1, stage2, 0), (1, stage2, 2)),
        2: ((2, stage5, 0), (3, stage7, 1), (2, stage5, 1)),
        3: ((1, stage3, 2), (1, stage3, 0), (3, stage7, 0), (2, stage5, 2), (3, stage7, 2),
            (3, store, 0), (3, stage8, 0)),
        4: ((3, stage8, 1), (3, stage8, 2), (3, store, 1), (1, stage3, 1)),
        5: ((3, stage9, 0), (1, stage4, 2), (2, stage6, 1)),
        6: ((1, stage4, 0),),
        7: ((1, stage4, 1),),
        8: ((2, stage6, 0),),
        9: ((2, stage6, 2),),
    }

    def at(i, pos):
        for lag, stage, k in plan.get(pos, ()):
            j = i - lag

            @pl.when((j >= 0) & (j < n))
            def _():
                stage(j, k)

    x_copy(0).start()
    for v in range(GS):
        for c in g_copies(v):
            c.start()
    barrier = pltpu.get_barrier_semaphore()
    for dev in [sib] + prts:
        pl.semaphore_signal(barrier, inc=1, device_id={"tp": dev}, device_id_type=MESH)
    pl.semaphore_wait(barrier, 4)

    def slot(i, carry):
        @pl.when(i < n)
        def _():
            x_copy(i).wait()

        @pl.when(i == n)
        def _():
            for h in range(2):
                t_copy(h).start()

        def gate_up(b, carry):
            @pl.when(i < n)
            def _():
                u = NG * i + b
                gate = up = 0.0
                for h in range(2):
                    v = 2 * u + h
                    for c in g_copies(v):
                        c.wait()
                    xh = xb[:, h * DH:(h + 1) * DH]
                    gate += jnp.dot(xh, wgb[v % GS], preferred_element_type=F32)
                    up += jnp.dot(xh, wub[v % GS], preferred_element_type=F32)

                    @pl.when((v + GS < 2 * NG * n) & ((i > 0) | (v + GS < 2 * NG)))
                    def _():
                        for c in g_copies(v + GS):
                            c.start()
                hid[:, pl.ds(mo(b * GB, GB), GB)] = (jax.nn.silu(gate) * up).astype(BF16)

                for p, ds in ((2, (0,)), (3, (1, 2, 3)), (4, (4, 5))):
                    @pl.when(u == p)
                    def _():
                        for d in ds:
                            d_copy(d).start()

                @pl.when((b == NG - 1) & (i > 0) & (i + 1 < n))
                def _():
                    x_copy(i + 1).start()

            for pos in range(NG):
                @pl.when(b == pos)
                def _():
                    at(i, pos)
            return carry

        lax.fori_loop(0, NG, gate_up, 0)

        def down(d):
            @pl.when(i == 0)
            def _():
                d_copy(d).wait()
            return jnp.dot(hid[...], wdb[d // 3, :, cols(d % 3)], preferred_element_type=F32)

        for d in range(3):
            @pl.when(i < n)
            def _():
                sb0[:, cols(d)] = down(d).astype(BF16)
                d2d0(i, d).start()
            at(i, NG + d)
            if d == 1:
                @pl.when(i == 0)
                def _():
                    x_copy(1).start()
                    for v in range(2 * NG, 2 * NG + GS):
                        for c in g_copies(v):
                            c.start()

        for k in range(3):
            @pl.when(i < n)
            def _():
                d2d0(i, k).wait_recv()
                own[:, cols(k)] = down(3 + k) + rb0[i % 2, :, cols(k)].astype(F32)
                stage1(i, k)
            at(i, NG + 3 + k)
        return carry

    lax.fori_loop(0, n + 3, slot, 0)
    for h in range(2):
        t_copy(h).wait()


def finish(n, wdb, yo, yb, y_hbm, sem):
    core = lax.axis_index("tp") % 2
    outs = []
    for j in range(n):
        for h in range(2):
            rows = pl.ds(j * M, M)
            if j < n - YS:
                src, half = wdb.at[h, rows, :], h
            else:
                src, half = (yo, yb)[h].at[j % YS], (core, 1 - core)[h]
            dst = y_hbm.at[rows, pl.ds(pl.multiple_of(half * HALF, 128), HALF)]
            outs.append(pltpu.make_async_copy(src, dst, sem.at[j, h]))
            outs[-1].start()
    for c in outs:
        c.wait()


def solution(mesh):
    def step(x, w_gate, w_up, w_down):
        n = x.shape[0] // M
        assert n > YS and (n - YS) * M <= FF
        dma = pltpu.SemaphoreType.DMA
        vmem = pl.BlockSpec(memory_space=pltpu.VMEM)
        part = pltpu.VMEM((YS, M, HALF), BF16)
        outs = pl.pallas_call(
            functools.partial(kernel, n),
            out_shape=(jax.ShapeDtypeStruct((2, (n - YS) * M, HALF), BF16),
                       pltpu.VMEM((2, FF, HALF), BF16), part, part),
            in_specs=[pl.BlockSpec(memory_space=pl.ANY)] * 4,
            out_specs=(pl.BlockSpec(memory_space=pl.ANY), vmem, vmem, vmem),
            scratch_shapes=[
                pltpu.VMEM((M, D), BF16),
                pltpu.VMEM((GS, DH, GB), BF16),
                pltpu.VMEM((GS, DH, GB), BF16),
                pltpu.VMEM((M, FF), BF16),
                pltpu.VMEM((M, HALF), BF16),
                pltpu.VMEM((2, M, HALF), BF16),
                pltpu.VMEM((M, HALF), F32),
                pltpu.VMEM((M // 2, HALF), BF16),
                pltpu.VMEM((2, M // 2, HALF), BF16),
                pltpu.VMEM((M // 4, HALF), BF16),
                pltpu.VMEM((2, M // 4, HALF), BF16),
                pltpu.VMEM((M // 8, HALF), BF16),
                pltpu.VMEM((2, M // 8, HALF), BF16),
                dma((1,)), dma((GS,)), dma((GS,)), dma((6,)), dma((2, YS)),
                dma((3,)), dma((2, 3)),
                dma((3, 3)), dma((2, 3, 3)),
                dma((3, 2)), dma((2, 3, 2)),
                dma((3,)), dma((2, 3)),
                dma((YS, 3, 7)), dma((YS, 3, 7)),
                dma((YS, 3, 2)), dma((YS, 3, 2)),
            ],
            compiler_params=pltpu.CompilerParams(
                collective_id=0, has_side_effects=True, vmem_limit_bytes=37_500_000),
            name="mlp_ring",
        )(x, w_gate, w_up, w_down)
        return pl.pallas_call(
            functools.partial(finish, n),
            out_shape=jax.ShapeDtypeStruct(x.shape, BF16),
            in_specs=[vmem] * 3,
            out_specs=pl.BlockSpec(memory_space=pl.ANY),
            scratch_shapes=[dma((n, 2))],
            compiler_params=pltpu.CompilerParams(vmem_limit_bytes=1_000_000),
            name="finish",
        )(*outs[1:])

    return jax.shard_map(
        step,
        mesh=mesh,
        in_specs=(P("dp", None), P(None, "tp"), P(None, "tp"), P("tp", None)),
        out_specs=P("dp", None),
        check_vma=False,
    )
```

```python
import functools

import jax
import jax.numpy as jnp
from jax import lax
from jax.experimental import pallas as pl
from jax.experimental.pallas import tpu as pltpu
from jax.sharding import PartitionSpec as P

D = 7168
FF = 1280
M = 256
HALF = D // 2
OFF = (0, 1280, 2432)
WID = (1280, 1152, 1152)
GB = 256
NG = FF // GB
DH = D // 2
GS = 3
PC = M // 8
YS = 3
MESH = pl.DeviceIdType.MESH
F32 = jnp.float32
BF16 = jnp.bfloat16


def kernel(n, x_hbm, wg_hbm, wu_hbm, wd_hbm, t_hbm, wdb, yo, yb,
           xb, wgb, wub, hid, sb0, rb0, own, s1, r1, s2, r2, s3, r3,
           xsem, gsem, usem, dsem, osem,
           ss0, rs0, ss1, rs1, ss2, rs2, ss3, rs3, ssg, rsg, ssd, rsd):
    me = lax.axis_index("tp")
    core = me % 2
    sib = me + 1 - 2 * core
    bits = [(me // s) % 2 for s in (2, 4, 8)]
    prts = [me + s - 2 * s * ((me // s) % 2) for s in (2, 4, 8)]

    def pick(vals, axis):
        return (vals[0] * ((1 - axis) * (2 - axis) // 2) + vals[1] * (axis * (2 - axis))
                + vals[2] * (axis * (axis - 1) // 2))

    def geo(j, k):
        out = []
        for t in range(3):
            axis = (j + core + k + t) % 3
            out.append((pick(bits, axis), pick(prts, axis)))
        return out

    def rc(src, dst, ssem, rsem, dev):
        return pltpu.make_async_remote_copy(
            src_ref=src, dst_ref=dst, send_sem=ssem, recv_sem=rsem,
            device_id={"tp": dev}, device_id_type=MESH)

    def cols(k):
        return pl.ds(OFF[k], WID[k])

    def mo(v, m):
        return pl.multiple_of(v, m)

    def x_copy(i):
        return pltpu.make_async_copy(
            x_hbm.at[pl.ds(mo(i * M, M), M), :], xb, xsem.at[0])

    def g_copies(v):
        c = pl.ds(mo((v // 2) % NG * GB, GB), GB)
        r = pl.ds(mo(v % 2 * DH, DH), DH)
        return (pltpu.make_async_copy(wg_hbm.at[r, c], wgb.at[v % GS], gsem.at[v % GS]),
                pltpu.make_async_copy(wu_hbm.at[r, c], wub.at[v % GS], usem.at[v % GS]))

    def d_copy(d):
        k = d % 3
        half = (1 - core) if d < 3 else core
        c = pl.ds(mo(half * HALF + OFF[k], 128), WID[k])
        return pltpu.make_async_copy(wd_hbm.at[:, c], wdb.at[d // 3, :, cols(k)], dsem.at[d])

    def y_copy(j, buf, half, which):
        return pltpu.make_async_copy(
            buf.at[j % YS], t_hbm.at[half, pl.ds(mo(j * M, M), M), :], osem.at[which, j % YS])

    def t_copy(h):
        r = (n - YS) * M
        return pltpu.make_async_copy(t_hbm.at[h], wdb.at[h, pl.ds(0, r), :], dsem.at[h])

    def d2d0(j, k):
        return rc(sb0.at[:, cols(k)], rb0.at[j % 2, :, cols(k)], ss0.at[k], rs0.at[j % 2, k], sib)

    def off1(g, p):
        (_, _), (bb, _), (bc, _) = g
        if p == 0:
            return mo((1 - bb) * 2 * PC, PC), 2 * PC
        if p == 1:
            return mo(bb * 2 * PC + (1 - bc) * PC, PC), PC
        return mo(bb * 2 * PC + bc * PC, PC), PC

    def c1(j, k, g, p):
        o, r = off1(g, p)
        return rc(s1.at[pl.ds(o, r), cols(k)], r1.at[j % 2, pl.ds(o, r), cols(k)],
                  ss1.at[k, p], rs1.at[j % 2, k, p], g[0][1])

    def off2(g, p):
        bc = g[2][0]
        return mo((1 - bc) * PC if p == 0 else bc * PC, PC)

    def c2(j, k, g, p):
        o = off2(g, p)
        return rc(s2.at[pl.ds(o, PC), cols(k)], r2.at[j % 2, pl.ds(o, PC), cols(k)],
                  ss2.at[k, p], rs2.at[j % 2, k, p], g[1][1])

    def c3(j, k, g):
        return rc(s3.at[:, cols(k)], r3.at[j % 2, :, cols(k)], ss3.at[k], rs3.at[j % 2, k], g[2][1])

    AG = (((0, 0, 0), 2), ((0, 0, 0), 1), ((0, 0, 0), 0),
          ((0, 0, 1), 1), ((0, 0, 1), 0), ((0, 1, 0), 0), ((0, 1, 1), 0))

    def off_g(g, f):
        v = 0
        for t, wgt in enumerate((4, 2, 1)):
            b = g[t][0]
            v = v + (1 - b if f[t] else b) * (wgt * PC)
        return mo(v, PC)

    def cg(j, k, g, q):
        f, t = AG[q]
        o = off_g(g, f)
        ref = yo.at[j % YS, pl.ds(o, PC), cols(k)]
        return rc(ref, ref, ssg.at[j % YS, k, q], rsg.at[j % YS, k, q], g[t][1])

    def cg_in(j, k, g, q):
        f, t = AG[q]
        f = tuple(1 - v if u == t else v for u, v in enumerate(f))
        o = off_g(g, f)
        ref = yo.at[j % YS, pl.ds(o, PC), cols(k)]
        return rc(ref, ref, ssg.at[j % YS, k, q], rsg.at[j % YS, k, q], g[t][1])

    def cd(j, k, g, p, mine=True):
        ba = g[0][0]
        o = mo((ba if p == 0 else 1 - ba) * 4 * PC, 4 * PC)
        return rc(yo.at[j % YS, pl.ds(o, 4 * PC), cols(k)], yb.at[j % YS, pl.ds(o, 4 * PC), cols(k)],
                  ssd.at[j % YS, k, p], rsd.at[j % YS, k, p], sib)

    def cd_in(j, k, p):
        return rc(yo.at[j % YS, pl.ds(0, 4 * PC), cols(k)], yb.at[j % YS, pl.ds(0, 4 * PC), cols(k)],
                  ssd.at[j % YS, k, p], rsd.at[j % YS, k, p], sib)

    def stage1(i, k):
        g = geo(i, k)
        ba = g[0][0]
        o = mo((1 - ba) * 4 * PC, 4 * PC)
        s1[:, cols(k)] = own[pl.ds(o, 4 * PC), cols(k)].astype(BF16)
        for p in range(3):
            c1(i, k, g, p).start()

    def own_rows(g, o, r):
        return pl.ds(mo(g[0][0] * 4 * PC + o, PC), r)

    def stage2(j, k):
        g = geo(j, k)
        o, r = off1(g, 0)
        c1(j, k, g, 0).wait_recv()
        s2[:, cols(k)] = (own[own_rows(g, o, r), cols(k)]
                          + r1[j % 2, pl.ds(o, r), cols(k)].astype(F32)).astype(BF16)
        for p in range(2):
            c2(j, k, g, p).start()
        d2d0(j, k).wait_send()

    def stage3(j, k):
        g = geo(j, k)
        o, r = off1(g, 1)
        c1(j, k, g, 1).wait_recv()
        c2(j, k, g, 0).wait_recv()
        s3[:, cols(k)] = (own[own_rows(g, o, r), cols(k)]
                          + r1[j % 2, pl.ds(o, r), cols(k)].astype(F32)
                          + r2[j % 2, pl.ds(off2(g, 0), PC), cols(k)].astype(F32)).astype(BF16)
        c3(j, k, g).start()

    def stage4(j, k):
        g = geo(j, k)
        o, r = off1(g, 2)
        c1(j, k, g, 2).wait_recv()
        c2(j, k, g, 1).wait_recv()
        c3(j, k, g).wait_recv()
        yo[j % YS, pl.ds(off_g(g, (0, 0, 0)), PC), cols(k)] = (
            own[own_rows(g, o, r), cols(k)]
            + r1[j % 2, pl.ds(o, r), cols(k)].astype(F32)
            + r2[j % 2, pl.ds(off2(g, 1), PC), cols(k)].astype(F32)
            + r3[j % 2, :, cols(k)].astype(F32)).astype(BF16)
        for q in range(3):
            cg(j, k, g, q).start()
        for p in range(3):
            c1(j, k, g, p).wait_send()
        for p in range(2):
            c2(j, k, g, p).wait_send()
        c3(j, k, g).wait_send()

    def stage5(j, k):
        g = geo(j, k)
        cg_in(j, k, g, 0).wait_recv()
        cg(j, k, g, 3).start()
        cg(j, k, g, 4).start()
        cg_in(j, k, g, 1).wait_recv()
        cg(j, k, g, 5).start()

    def stage6(j, k):
        g = geo(j, k)
        cg_in(j, k, g, 3).wait_recv()
        cg(j, k, g, 6).start()
        cd(j, k, g, 0).start()

    def stage7(j, k):
        g = geo(j, k)
        for q in (2, 4, 5, 6):
            cg_in(j, k, g, q).wait_recv()
        cd(j, k, g, 1).start()

    def stage8(j, k):
        for p in range(2):
            cd_in(j, k, p).wait_recv()

    def store(j, which):
        @pl.when(j < n - YS)
        def _():
            y_copy(j, (yo, yb)[which], (core, 1 - core)[which], which).start()

    def stage9(j, _):
        for k in range(3):
            g = geo(j, k)
            for q in range(7):
                cg(j, k, g, q).wait_send()
            for p in range(2):
                cd(j, k, g, p).wait_send()

        @pl.when(j < n - YS)
        def _():
            y_copy(j, yo, core, 0).wait()
            y_copy(j, yb, 1 - core, 1).wait()

    plan = {
        1: ((1, stage2, 0), (1, stage2, 1), (3, stage7, 1), (1, stage2, 2)),
        2: ((2, stage5, 0), (2, stage5, 1), (3, stage7, 0)),
        3: ((1, stage3, 2), (3, stage7, 2), (1, stage3, 0), (2, stage5, 2), (1, stage3, 1),
            (3, store, 0)),
        4: ((3, stage8, 2), (3, stage8, 1), (3, stage8, 0), (3, store, 1)),
        5: ((3, stage9, 0), (1, stage4, 2), (2, stage6, 1)),
        6: ((1, stage4, 0),),
        7: ((1, stage4, 1), (2, stage6, 0)),
        8: ((2, stage6, 2),),
    }

    def at(i, pos):
        for lag, stage, k in plan.get(pos, ()):
            j = i - lag

            @pl.when((j >= 0) & (j < n))
            def _():
                stage(j, k)

    x_copy(0).start()
    for v in range(GS):
        for c in g_copies(v):
            c.start()
    barrier = pltpu.get_barrier_semaphore()
    for dev in [sib] + prts:
        pl.semaphore_signal(barrier, inc=1, device_id={"tp": dev}, device_id_type=MESH)
    pl.semaphore_wait(barrier, 4)

    def slot(i, carry):
        @pl.when(i < n)
        def _():
            x_copy(i).wait()

        @pl.when(i == n)
        def _():
            for h in range(2):
                t_copy(h).start()

        def gate_up(b, carry):
            @pl.when(i < n)
            def _():
                u = NG * i + b
                gate = up = 0.0
                for h in range(2):
                    v = 2 * u + h
                    for c in g_copies(v):
                        c.wait()
                    xh = xb[:, h * DH:(h + 1) * DH]
                    gate += jnp.dot(xh, wgb[v % GS], preferred_element_type=F32)
                    up += jnp.dot(xh, wub[v % GS], preferred_element_type=F32)

                    @pl.when((v + GS < 2 * NG * n) & ((i > 0) | (v + GS < 2 * NG)))
                    def _():
                        for c in g_copies(v + GS):
                            c.start()
                hid[:, pl.ds(mo(b * GB, GB), GB)] = (jax.nn.silu(gate) * up).astype(BF16)

                for p, ds in ((2, (0,)), (3, (1, 2, 3)), (4, (4, 5))):
                    @pl.when(u == p)
                    def _():
                        for d in ds:
                            d_copy(d).start()

                @pl.when((b == NG - 1) & (i > 0) & (i + 1 < n))
                def _():
                    x_copy(i + 1).start()

            for pos in range(NG):
                @pl.when(b == pos)
                def _():
                    at(i, pos)
            return carry

        lax.fori_loop(0, NG, gate_up, 0)

        def down(d):
            @pl.when(i == 0)
            def _():
                d_copy(d).wait()
            return jnp.dot(hid[...], wdb[d // 3, :, cols(d % 3)], preferred_element_type=F32)

        for d in range(3):
            @pl.when(i < n)
            def _():
                sb0[:, cols(d)] = down(d).astype(BF16)
                d2d0(i, d).start()
            at(i, NG + d)
            if d == 1:
                @pl.when(i == 0)
                def _():
                    x_copy(1).start()
                    for v in range(2 * NG, 2 * NG + GS):
                        for c in g_copies(v):
                            c.start()

        for k in range(3):
            @pl.when(i < n)
            def _():
                d2d0(i, k).wait_recv()
                own[:, cols(k)] = down(3 + k) + rb0[i % 2, :, cols(k)].astype(F32)
                stage1(i, k)
            at(i, NG + 3 + k)
        return carry

    lax.fori_loop(0, n + 3, slot, 0)
    for h in range(2):
        t_copy(h).wait()


def finish(n, wdb, yo, yb, y_hbm, sem):
    core = lax.axis_index("tp") % 2
    outs = []
    for j in range(n):
        for h in range(2):
            rows = pl.ds(j * M, M)
            if j < n - YS:
                src, half = wdb.at[h, rows, :], h
            else:
                src, half = (yo, yb)[h].at[j % YS], (core, 1 - core)[h]
            dst = y_hbm.at[rows, pl.ds(pl.multiple_of(half * HALF, 128), HALF)]
            outs.append(pltpu.make_async_copy(src, dst, sem.at[j, h]))
            outs[-1].start()
    for c in outs:
        c.wait()


def solution(mesh):
    def step(x, w_gate, w_up, w_down):
        n = x.shape[0] // M
        assert n > YS and (n - YS) * M <= FF
        dma = pltpu.SemaphoreType.DMA
        vmem = pl.BlockSpec(memory_space=pltpu.VMEM)
        part = pltpu.VMEM((YS, M, HALF), BF16)
        outs = pl.pallas_call(
            functools.partial(kernel, n),
            out_shape=(jax.ShapeDtypeStruct((2, (n - YS) * M, HALF), BF16),
                       pltpu.VMEM((2, FF, HALF), BF16), part, part),
            in_specs=[pl.BlockSpec(memory_space=pl.ANY)] * 4,
            out_specs=(pl.BlockSpec(memory_space=pl.ANY), vmem, vmem, vmem),
            scratch_shapes=[
                pltpu.VMEM((M, D), BF16),
                pltpu.VMEM((GS, DH, GB), BF16),
                pltpu.VMEM((GS, DH, GB), BF16),
                pltpu.VMEM((M, FF), BF16),
                pltpu.VMEM((M, HALF), BF16),
                pltpu.VMEM((2, M, HALF), BF16),
                pltpu.VMEM((M, HALF), F32),
                pltpu.VMEM((M // 2, HALF), BF16),
                pltpu.VMEM((2, M // 2, HALF), BF16),
                pltpu.VMEM((M // 4, HALF), BF16),
                pltpu.VMEM((2, M // 4, HALF), BF16),
                pltpu.VMEM((M // 8, HALF), BF16),
                pltpu.VMEM((2, M // 8, HALF), BF16),
                dma((1,)), dma((GS,)), dma((GS,)), dma((6,)), dma((2, YS)),
                dma((3,)), dma((2, 3)),
                dma((3, 3)), dma((2, 3, 3)),
                dma((3, 2)), dma((2, 3, 2)),
                dma((3,)), dma((2, 3)),
                dma((YS, 3, 7)), dma((YS, 3, 7)),
                dma((YS, 3, 2)), dma((YS, 3, 2)),
            ],
            compiler_params=pltpu.CompilerParams(
                collective_id=0, has_side_effects=True, vmem_limit_bytes=37_500_000),
            name="mlp_ring",
        )(x, w_gate, w_up, w_down)
        return pl.pallas_call(
            functools.partial(finish, n),
            out_shape=jax.ShapeDtypeStruct(x.shape, BF16),
            in_specs=[vmem] * 3,
            out_specs=pl.BlockSpec(memory_space=pl.ANY),
            scratch_shapes=[dma((n, 2))],
            compiler_params=pltpu.CompilerParams(vmem_limit_bytes=1_000_000),
            name="finish",
        )(*outs[1:])

    return jax.shard_map(
        step,
        mesh=mesh,
        in_specs=(P("dp", None), P(None, "tp"), P(None, "tp"), P("tp", None)),
        out_specs=P("dp", None),
        check_vma=False,
    )
```
